32 devices in a mesh: asset: 8 (over y, x, core), tm: 4 (over z).
Axes of the slice: x: 2, y: 2, z: 4, core: 2. Of those that a mesh axis runs over, the one named last changes fastest.
Arguments:
- day_ranks: int32 [144, 4096], P('tm', 'asset'), may hold values from 2 to 240
- confidence: float32 [144, 4096], P('tm', 'asset'), may hold values from 0.25 to 4
Outputs:
- correlation: bfloat16 [24, 4096, 4096], P('tm', 'asset')
The draws below stay inside these ranges and needn't reach their ends.
All inputs are finite; a program needn't handle non-finite values.
Results may differ from the reference program's by a relative error of at most 0.001.
Values sent between devices are 32-bit elements; how exact they have to be, the bound alone decides.
No kernel may reach another device: no remote copies, remote signals or barrier semaphores. Data moves between devices by JAX's collectives and lax.ppermute only.
A program may use at most 64 MiB of HBM per device.

```python
import math
import jax
import jax.numpy as jnp
from jax import lax

ASSETS = 4096
WIN = 120
DAYS = 144
ENDS = 24
LEAD = 1


def touch_ends(values, key, low, high):
    index_at = [jax.random.randint(jax.random.fold_in(key, axis), (), 0, length) for axis, length in enumerate(values.shape)]
    longest = values.shape.index(max(values.shape))
    next_to = index_at[:longest] + [(index_at[longest] + 1) % values.shape[longest]] + index_at[longest + 1:]
    return values.at[tuple(index_at)].set(low).at[tuple(next_to)].set(high)


def shard_levels(key, extent, pieces, least, high):
    def one(dim, parts):
        steps = jax.random.uniform(jax.random.fold_in(jax.random.fold_in(key, 6), dim), (parts,), jnp.float32, least / len(pieces), high / len(pieces))
        return jnp.repeat(jnp.exp(steps), extent[dim] // parts).reshape((-1,) + (1,) * (len(extent) - dim - 1))

    level = one(*pieces[0])
    for cut in pieces[1:]:
        level = level * one(*cut)
    return level


def setup_inputs(seed: int = 0) -> dict:
    key_list = jax.random.split(jax.random.key(seed), 3)
    day_ranks = touch_ends(jax.random.randint(key_list[0], (DAYS, ASSETS), 2, 2 * WIN + 1), jax.random.fold_in(key_list[0], 1), 2, 2 * WIN).astype(jnp.int32)
    confidence = jnp.clip(jnp.exp(math.log(4.0) - 2.7725887 * jax.random.uniform(key_list[1], (DAYS, ASSETS), jnp.float32) ** shard_levels(key_list[1], (DAYS, ASSETS), ((0, 4), (1, 8)), -0.2, 0.2)), 0.25, 4.0)
    return {"day_ranks": day_ranks, "confidence": confidence}


epsilon = 1e-06

def reference(day_ranks, confidence):
    scores = confidence * (day_ranks - (WIN + 1)).astype(jnp.float32) / WIN

    def end_correlation(end_index):
        window_rows = lax.dynamic_slice_in_dim(scores, (end_index + LEAD).astype(jnp.int32), WIN, 0)
        window_mean = lax.optimization_barrier(jnp.sum(window_rows, 0)) / WIN
        centred = window_rows - window_mean[None, :]
        window_scale = lax.rsqrt(lax.optimization_barrier(jnp.sum(centred * centred, 0)) / WIN + epsilon)
        gram_sums = jnp.dot(window_rows.T, window_rows, precision=lax.Precision.HIGHEST, preferred_element_type=jnp.float32)
        centre = window_mean[:, None] * window_mean[None, :]
        spread = window_scale[:, None] * window_scale[None, :]
        return ((gram_sums / WIN - centre) * spread).astype(jnp.bfloat16)
    return lax.map(end_correlation, jnp.arange(ENDS, dtype=jnp.int32))
```

```python
import jax
import jax.numpy as jnp
from jax import lax
from jax.experimental import pallas as pl
from jax.experimental.pallas import tpu as pltpu
from jax.sharding import PartitionSpec as P


WIN = 120
ENDS_DEV = 6
ROWS = 128
EDGE = 16


epsilon = 1e-06


def window_stats(span, offset):
    rows, width = span.shape
    inner = rows - 2 * EDGE
    centre = jnp.sum(span[EDGE : rows - EDGE], 0, keepdims=True) * (1.0 / inner)
    shifted = span - centre
    middle = shifted[EDGE : rows - EDGE]
    middle_sum = jnp.sum(middle, 0, keepdims=True)
    middle_square = jnp.sum(middle * middle, 0, keepdims=True)
    edge = jnp.concatenate([shifted[:EDGE], shifted[rows - EDGE :]], 0)
    edge_square = edge * edge
    row = lax.broadcasted_iota(jnp.int32, (2 * EDGE, width), 0)
    day = jnp.where(row < EDGE, row, row + inner) - offset
    means, scales = [], []
    for end in range(ENDS_DEV):
        inside = (day >= end) & (day < end + WIN)
        total = middle_sum + jnp.sum(jnp.where(inside, edge, 0.0), 0, keepdims=True)
        square = middle_square + jnp.sum(jnp.where(inside, edge_square, 0.0), 0, keepdims=True)
        mean = total / WIN
        means.append(mean)
        scales.append(lax.rsqrt(square / WIN - mean * mean + epsilon))
    return shifted, means, scales


def split(value):
    high = value.astype(jnp.bfloat16)
    return high, (value - high.astype(jnp.float32)).astype(jnp.bfloat16)


def left_kernel(index_ref, span_ref, left_ref):
    offset = index_ref[0]
    shifted, means, scales = window_stats(span_ref[...], offset)
    rows, width = shifted.shape
    filler = jnp.zeros((16 - 2 * ENDS_DEV, width), jnp.float32)
    columns = jnp.concatenate(means + scales + [filler], 0).T
    turned = shifted.T
    day = lax.broadcasted_iota(jnp.int32, (width, rows), 1) - offset
    for end in range(ENDS_DEV):
        mean = columns[:, end : end + 1]
        scale = columns[:, ENDS_DEV + end : ENDS_DEV + end + 1]
        inside = (day >= end) & (day < end + WIN)
        high, low = split(jnp.where(inside, (turned - mean) * (scale / WIN), 0.0))
        left_ref[end, :, 0:rows] = high
        left_ref[end, :, rows : 2 * rows] = high
        left_ref[end, :, 2 * rows : 3 * rows] = low


def left_factors(index, span):
    rows, width = span.shape
    return pl.pallas_call(
        left_kernel,
        out_shape=jax.ShapeDtypeStruct((ENDS_DEV, width, 3 * rows), jnp.bfloat16),
        in_specs=[pl.BlockSpec(memory_space=pltpu.SMEM), pl.BlockSpec(memory_space=pltpu.VMEM)],
        out_specs=pl.BlockSpec(memory_space=pltpu.VMEM),
        compiler_params=pltpu.CompilerParams(vmem_limit_bytes=12 << 20),
        cost_estimate=pl.CostEstimate(flops=6000000000, bytes_accessed=0, transcendentals=0),
        name="left_factors",
    )(index, span)


def tile_kernel(index_ref, left_ref, *refs, blocks):
    spans = refs[:blocks]
    output_ref, tile_ref, sem = refs[-3:]
    width = spans[0].shape[1]
    copies = []
    for block in range(blocks):
        shifted, _, scales = window_stats(spans[block][...], index_ref[0])
        high, low = split(shifted)
        right = jnp.concatenate([high, low, high], 0)
        column = index_ref[1 + block] * width
        for end in range(ENDS_DEV):
            gram = jnp.dot(left_ref[end], right, preferred_element_type=jnp.float32)
            tile_ref[block, end] = (gram * scales[end]).astype(jnp.bfloat16)
            copy = pltpu.make_async_copy(
                tile_ref.at[block, end],
                output_ref.at[end, :, pl.ds(column, width)],
                sem.at[block, end],
            )
            copy.start()
            copies.append(copy)
    for copy in copies:
        copy.wait()


def tiles(index, left, spans, output, output_shape):
    blocks = len(spans)
    ends, height, _ = left.shape
    width = spans[0].shape[1]
    args = [index, left, *spans]
    specs = [pl.BlockSpec(memory_space=pltpu.SMEM)] + [pl.BlockSpec(memory_space=pltpu.VMEM)] * (1 + blocks)
    aliases = {}
    if output is not None:
        aliases = {len(args): 0}
        args.append(output)
        specs.append(pl.BlockSpec(memory_space=pl.ANY))
    return pl.pallas_call(
        lambda *refs: tile_kernel(*refs, blocks=blocks),
        out_shape=jax.ShapeDtypeStruct(output_shape, jnp.bfloat16),
        in_specs=specs,
        out_specs=pl.BlockSpec(memory_space=pl.ANY),
        scratch_shapes=[
            pltpu.VMEM((blocks, ends, height, width), jnp.bfloat16),
            pltpu.SemaphoreType.DMA((blocks, ends)),
        ],
        input_output_aliases=aliases,
        compiler_params=pltpu.CompilerParams(vmem_limit_bytes=20 << 20),
        cost_estimate=pl.CostEstimate(flops=12000000000, bytes_accessed=0, transcendentals=0),
        name="tiles",
    )(*args)


def partner(value, bits):
    pairs = [(source, source ^ bits) for source in range(lax.axis_size("asset"))]
    return lax.ppermute(value, "asset", pairs)


def correlations(day_ranks, confidence):
    days_dev, width = day_ranks.shape
    time_count = lax.axis_size("tm")
    asset_count = lax.axis_size("asset")
    days = days_dev * time_count
    lead_days = days - ENDS_DEV * time_count - WIN + 1
    time_index = lax.axis_index("tm")
    own_index = lax.axis_index("asset")
    first_day = lead_days + time_index * ENDS_DEV
    start = jnp.minimum(first_day, days - ROWS)
    offset = first_day - start

    scores = confidence * (day_ranks - (WIN + 1)).astype(jnp.float32) / WIN
    all_days = jnp.zeros((days, width), jnp.float32)
    for steps in range(time_count):
        shard = scores
        if steps:
            pairs = [(source, source ^ steps) for source in range(time_count)]
            shard = lax.ppermute(scores, "tm", pairs)
        place = (time_index ^ steps) * days_dev
        all_days = lax.dynamic_update_slice_in_dim(all_days, shard, place, 0)
    span = lax.dynamic_slice_in_dim(all_days, start, ROWS, 0)

    hops = range(0, asset_count, 2)
    arrived = {0: span}
    for bits in hops[1:]:
        arrived[bits] = partner(span, bits)
    left = left_factors(jnp.stack([offset]).astype(jnp.int32), span)
    output = None
    for bits in hops:
        pair = [arrived[bits], partner(arrived[bits], 1)]
        index = jnp.stack([offset, own_index ^ bits, own_index ^ bits ^ 1]).astype(jnp.int32)
        output = tiles(index, left, pair, output, (ENDS_DEV, width, width * asset_count))
    return output


def solution(mesh):
    return jax.shard_map(
        correlations,
        mesh=mesh,
        in_specs=(P("tm", "asset"), P("tm", "asset")),
        out_specs=P("tm", "asset", None),
        check_vma=False,
    )
```

```python
import jax
import jax.numpy as jnp
from jax import lax
from jax.experimental import pallas as pl
from jax.experimental.pallas import tpu as pltpu
from jax.sharding import PartitionSpec as P


WIN = 120
ENDS_DEV = 6
ROWS = 128
EDGE = 16


epsilon = 1e-06


def window_stats(span, offset):
    rows, width = span.shape
    inner = rows - 2 * EDGE
    centre = jnp.sum(span[EDGE : rows - EDGE], 0, keepdims=True) * (1.0 / inner)
    shifted = span - centre
    middle = shifted[EDGE : rows - EDGE]
    middle_sum = jnp.sum(middle, 0, keepdims=True)
    middle_square = jnp.sum(middle * middle, 0, keepdims=True)
    edge = jnp.concatenate([shifted[:EDGE], shifted[rows - EDGE :]], 0)
    edge_square = edge * edge
    row = lax.broadcasted_iota(jnp.int32, (2 * EDGE, width), 0)
    day = jnp.where(row < EDGE, row, row + inner) - offset
    means, scales = [], []
    for end in range(ENDS_DEV):
        inside = (day >= end) & (day < end + WIN)
        total = middle_sum + jnp.sum(jnp.where(inside, edge, 0.0), 0, keepdims=True)
        square = middle_square + jnp.sum(jnp.where(inside, edge_square, 0.0), 0, keepdims=True)
        mean = total / WIN
        means.append(mean)
        scales.append(lax.rsqrt(square / WIN - mean * mean + epsilon))
    return shifted, means, scales


def span_place(days):
    time_count = lax.axis_size("tm")
    first_day = days - ENDS_DEV * time_count - WIN + 1 + lax.axis_index("tm") * ENDS_DEV
    start = jnp.minimum(first_day, days - ROWS)
    return start, first_day - start


def split(value):
    high = value.astype(jnp.bfloat16)
    return high, (value - high.astype(jnp.float32)).astype(jnp.bfloat16)


def span_kernel(*refs, days):
    *shard_refs, span_ref, days_ref = refs
    start, _ = span_place(days)
    time_index = lax.axis_index("tm")
    shards = [ref[...] for ref in shard_refs]
    for bit in range(len(shards).bit_length() - 1):
        swap = (time_index >> bit) % 2 == 1
        shards = [jnp.where(swap, shards[place ^ (1 << bit)], shards[place]) for place in range(len(shards))]
    days_ref[:days] = jnp.concatenate(shards, 0)
    rest = start % 8
    around = days_ref[pl.ds(pl.multiple_of(start - rest, 8), ROWS + 8), :]
    span_ref[...] = pltpu.roll(around, (ROWS + 8 - rest) % (ROWS + 8), 0)[:ROWS]


def span_of(shards, days):
    width = shards[0].shape[1]
    return pl.pallas_call(
        lambda *refs: span_kernel(*refs, days=days),
        out_shape=jax.ShapeDtypeStruct((ROWS, width), jnp.float32),
        in_specs=[pl.BlockSpec(memory_space=pltpu.VMEM)] * len(shards),
        out_specs=pl.BlockSpec(memory_space=pltpu.VMEM),
        scratch_shapes=[pltpu.VMEM((days + 8, width), jnp.float32)],
        compiler_params=pltpu.CompilerParams(vmem_limit_bytes=4 << 20),
        name="span",
    )(*shards)


def mean_rows(parts, width):
    return jnp.concatenate(parts + [jnp.zeros((2 * ROWS // 4 - len(parts), width), jnp.float32)], 0)


def left_kernel(span_ref, left_ref, scale_ref, *, days):
    _, offset = span_place(days)
    shifted, means, scales = window_stats(span_ref[...], offset)
    rows, width = shifted.shape
    high, low = [half.astype(jnp.float32) for half in split(shifted)]
    parts = []
    for mean in means:
        mean_high, mean_low = [half.astype(jnp.float32) for half in split(mean * -WIN)]
        parts += [mean_high, mean_high, mean_low]
    extra = jnp.concatenate(
        [high[:EDGE], low[:EDGE], mean_rows(parts, width), low[rows - EDGE :], high[rows - EDGE :]], 0
    )
    columns = jnp.concatenate(scales + [jnp.zeros((8 - ENDS_DEV, width), jnp.float32)], 0).T
    high, low = split(shifted.T)
    high = high.astype(jnp.float32)
    low = low.astype(jnp.float32)
    extra = extra.T
    lane = lax.broadcasted_iota(jnp.int32, (1, rows), 1)
    inner = ((lane >= EDGE) & (lane < rows - EDGE)).astype(jnp.float32)
    left_ref[ENDS_DEV, :, 0:rows] = (high * inner).astype(jnp.bfloat16)
    left_ref[ENDS_DEV, :, rows : 2 * rows] = (low * inner).astype(jnp.bfloat16)
    day = lane - offset
    near = jnp.where((lane >= EDGE) & (lane < 2 * EDGE), lane - EDGE, lane)
    near = jnp.where((lane >= rows - 2 * EDGE) & (lane < rows - EDGE), lane + EDGE, near) - offset
    spread = (lane >= 2 * EDGE) & (lane < rows - 2 * EDGE)
    for end in range(ENDS_DEV):
        first = 2 * EDGE + 3 * end
        inside = ((day >= end) & (day < end + WIN)).astype(jnp.float32)
        edges = ((near >= end) & (near < end + WIN)).astype(jnp.float32)
        edges = jnp.where(spread, ((lane >= first) & (lane < first + 3)).astype(jnp.float32), edges)
        left_ref[end, :, 0:rows] = (high * inside).astype(jnp.bfloat16)
        left_ref[end, :, rows : 2 * rows] = (extra * edges).astype(jnp.bfloat16)
        scale_ref[end] = jnp.broadcast_to(columns[:, end : end + 1] / WIN, (width, 128))


def left_factors(span, days):
    rows, width = span.shape
    return pl.pallas_call(
        lambda *refs: left_kernel(*refs, days=days),
        out_shape=(
            jax.ShapeDtypeStruct((ENDS_DEV + 1, width, 2 * rows), jnp.bfloat16),
            jax.ShapeDtypeStruct((ENDS_DEV, width, 128), jnp.float32),
        ),
        in_specs=[pl.BlockSpec(memory_space=pltpu.VMEM)],
        out_specs=[pl.BlockSpec(memory_space=pltpu.VMEM)] * 2,
        compiler_params=pltpu.CompilerParams(vmem_limit_bytes=12 << 20),
        cost_estimate=pl.CostEstimate(flops=6000000000, bytes_accessed=0, transcendentals=0),
        name="left_factors",
    )(span)


def tile_kernel(left_ref, scale_ref, *refs, partners, days):
    blocks = len(partners)
    spans = refs[:blocks]
    own_index = lax.axis_index("asset")
    _, offset = span_place(days)
    output_ref, tile_ref, base_ref, sem = refs[-4:]
    rows, width = spans[0].shape
    copies = []
    for block in range(blocks):
        shifted, means, scales = window_stats(spans[block][...], offset)
        high, low = split(shifted)
        parts = []
        for mean in means:
            mean_high, mean_low = split(mean)
            mean_high, mean_low = mean_high.astype(jnp.float32), mean_low.astype(jnp.float32)
            parts += [mean_high, mean_low, mean_high]
        middle = mean_rows(parts, width).astype(jnp.bfloat16)
        right = jnp.concatenate(
            [high, low[:EDGE], high[:EDGE], middle, high[rows - EDGE :], low[rows - EDGE :]], 0
        )
        base_ref[...] = jnp.dot(
            left_ref[ENDS_DEV], jnp.concatenate([low, high], 0), preferred_element_type=jnp.float32
        )
        column = (own_index ^ partners[block]) * width
        for end in range(ENDS_DEV):
            gram = jnp.dot(left_ref[end], right, preferred_element_type=jnp.float32)
            for at in range(0, width, 128):
                lanes = slice(at, at + 128)
                covariance = base_ref[:, lanes] + gram[:, lanes]
                tile_ref[block, end, :, lanes] = (covariance * scale_ref[end] * scales[end][:, lanes]).astype(
                    jnp.bfloat16
                )
            copy = pltpu.make_async_copy(
                tile_ref.at[block, end],
                output_ref.at[end, :, pl.ds(column, width)],
                sem.at[block, end],
            )
            copy.start()
            copies.append(copy)
    for copy in copies:
        copy.wait()


def tiles(left, spans, output, output_shape, days):
    left, scale = left
    partners, spans = zip(*spans.items())
    blocks = len(spans)
    _, height, _ = left.shape
    width = spans[0].shape[1]
    args = [left, scale, *spans]
    specs = [pl.BlockSpec(memory_space=pltpu.VMEM)] * (2 + blocks)
    aliases = {}
    if output is not None:
        aliases = {len(args): 0}
        args.append(output)
        specs.append(pl.BlockSpec(memory_space=pl.ANY))
    return pl.pallas_call(
        lambda *refs: tile_kernel(*refs, partners=partners, days=days),
        out_shape=jax.ShapeDtypeStruct(output_shape, jnp.bfloat16),
        in_specs=specs,
        out_specs=pl.BlockSpec(memory_space=pl.ANY),
        scratch_shapes=[
            pltpu.VMEM((blocks, ENDS_DEV, height, width), jnp.bfloat16),
            pltpu.VMEM((height, width), jnp.float32),
            pltpu.SemaphoreType.DMA((blocks, ENDS_DEV)),
        ],
        input_output_aliases=aliases,
        compiler_params=pltpu.CompilerParams(vmem_limit_bytes=20 << 20),
        cost_estimate=pl.CostEstimate(flops=12000000000, bytes_accessed=0, transcendentals=0),
        name="tiles",
    )(*args)


def partner(value, bits):
    pairs = [(source, source ^ bits) for source in range(lax.axis_size("asset"))]
    return lax.ppermute(value, "asset", pairs)


def steps_of(asset_count):
    order = [0, 1, *range(2, asset_count)]
    cuts = sorted({0, 2, *range(3, asset_count, 2), asset_count - 2, asset_count})
    return [order[low:high] for low, high in zip(cuts, cuts[1:])]


def correlations(day_ranks, confidence):
    days_dev, width = day_ranks.shape
    time_count = lax.axis_size("tm")
    asset_count = lax.axis_size("asset")
    days = days_dev * time_count
    scores = confidence * (day_ranks - (WIN + 1)).astype(jnp.float32) / WIN
    shards = [scores]
    for steps in range(1, time_count):
        shards.append(lax.ppermute(scores, "tm", [(source, source ^ steps) for source in range(time_count)]))
    span = span_of(shards, days)

    arrived = {0: span}
    for bits in range(2, asset_count, 2):
        arrived[bits] = partner(span, bits)
    left = left_factors(span, days)
    for bits in range(0, asset_count, 2):
        arrived[bits ^ 1] = partner(arrived[bits], 1)
    output = None
    for blocks in steps_of(asset_count):
        spans = {bits: arrived[bits] for bits in blocks}
        output = tiles(left, spans, output, (ENDS_DEV, width, width * asset_count), days)
    return output


def solution(mesh):
    return jax.shard_map(
        correlations,
        mesh=mesh,
        in_specs=(P("tm", "asset"), P("tm", "asset")),
        out_specs=P("tm", "asset", None),
        check_vma=False,
    )
```
